128 devices in a mesh: row: 8 (over x, core), col: 16 (over z, y).
Axes of the slice: x: 4, y: 4, z: 4, core: 2. Of those that a mesh axis runs over, the one named last changes fastest.
Arguments:
- velocity: float32 [3, 32, 2048, 1024], P(None, None, 'col', 'row'), may hold values from -6 to 6
- z_inverse: float32 [1024, 1024], replicated, may hold values from -0.1875 to 0.1875
- tiles: int32 [1024, 4], P(('row', 'col')), may hold values from 0 to 8191, as said below
- amplitude: float32 [1024, 4, 256], P(('row', 'col')), may hold values from -3 to 3
- lateral: float32 [1024, 8, 256], P(('row', 'col')), may hold values from -2 to 2
- vertical: float32 [1024, 128, 256], P(('row', 'col')), may hold values from -0.5 to 0.5
- wall_velocity: float32 [1024, 3, 256], P(('row', 'col')), may hold values from -6 to 6
- surface: float32 [1024, 256], P(('row', 'col')), may hold values from 0.5 to 2
Outputs:
- spectrum: float32 [2, 3, 32, 1024, 1024], P(None, None, 'row', 'col')
- marker_force: float32 [1024, 3, 256], P(('row', 'col'))
The draws below stay inside these ranges and needn't reach their ends.
Inputs may be any that keep to these rules, and one draw needn't show every extreme that they name: tiles[b, k] is a tile id in block b's row group; the column index holding tile t is t // 512. Among the 32 entries of one device's blocks, at most 8 (repeats counted) name tiles held by one column index.
All inputs are finite; a program needn't handle non-finite values.
Results may differ from the reference program's by a relative error of at most 0.000071.
Values sent between devices are 32-bit elements; how exact they have to be, the bound alone decides.
A program may use at most 128 MiB of HBM per device.

```python
import math
import jax
import jax.numpy as jnp
from jax import lax

NY = 2048
NZ = 1024
TY = 8
K = 4
BLOCK = 256
BLK_DEV = 8
XW = 32
TZ = 128
YTD = 16
T_DEV = 512
BLOCKS = 1024
N_ROW = 8
N_COL = 16


def draw_tiles(key, part):
    devices = N_ROW * N_COL
    request_count = BLK_DEV * K
    keys = jax.random.split(key, 4)
    hot_column = jax.random.randint(keys[0], (N_ROW,), 0, N_COL)
    hot_device = jnp.repeat(hot_column, N_COL)
    columns = jnp.arange(N_COL, dtype=jnp.int32)[None, :]
    scores = jax.random.randint(keys[1], (devices, N_COL), 0, 1 << 20) * N_COL + columns
    scores = jnp.where(columns == hot_device[:, None], (1 << 20) * N_COL + N_COL, scores)
    chosen = jnp.argsort(-scores, axis=1)[:, :4]

    def shuffled(one_key):
        return jax.random.permutation(one_key, request_count)
    order = jax.vmap(shuffled)(jax.random.split(keys[2], devices))
    holder = jnp.take_along_axis(chosen, order % 4, axis=1)
    within = jax.random.randint(keys[3], (devices, request_count), 0, T_DEV)
    return (holder * T_DEV + within).astype(jnp.int32).reshape(devices * BLK_DEV, K)


def levels(own_key, dims, cuts, smallest, high):
    loudness = 1.0
    for dim, shards_of in cuts:
        steps = jax.random.uniform(jax.random.fold_in(jax.random.fold_in(own_key, 6), dim), (shards_of,), jnp.float32, smallest / len(cuts), high / len(cuts))
        loudness = loudness * jnp.repeat(jnp.exp(steps), dims[dim] // shards_of).reshape((-1,) + (1,) * (len(dims) - 1 - dim))
    return loudness


def scatter_about(rng, dims, width, reach, cuts=(), kind=jnp.bfloat16):
    drawn = jax.random.normal(rng, dims, jnp.float32) * width
    if len(cuts) > 0:
        drawn = levels(rng, dims, cuts, -0.22, 0.18) * drawn
    return jnp.clip(drawn, min=-reach, max=reach).astype(kind)


def setup_inputs(seed: int = 0) -> dict:
    key_of = jax.random.split(jax.random.key(seed), 9)
    return {
        "velocity": scatter_about(key_of[0], (3, XW, NY, NZ), 1.0, 6.0, ((2, 16), (3, 8)), jnp.float32),
        "z_inverse": scatter_about(key_of[1], (NZ, NZ), NZ ** -0.5, 0.1875, (), jnp.float32),
        "tiles": draw_tiles(jax.random.fold_in(key_of[8], 71), 0),
        "amplitude": scatter_about(key_of[3], (BLOCKS, K, BLOCK), K ** -0.5, 3.0, ((0, 128),), jnp.float32),
        "lateral": scatter_about(key_of[4], (BLOCKS, TY, BLOCK), TY ** -0.5, 2.0, ((0, 128),), jnp.float32),
        "vertical": scatter_about(key_of[5], (BLOCKS, TZ, BLOCK), TZ ** -0.5, 0.5, ((0, 128),), jnp.float32),
        "wall_velocity": scatter_about(key_of[6], (BLOCKS, 3, BLOCK), 1.0, 6.0, ((0, 128),), jnp.float32),
        "surface": jnp.clip(jnp.exp(math.log(2.0) - 1.3862944 * jax.random.uniform(key_of[7], (BLOCKS, BLOCK), jnp.float32) ** levels(key_of[7], (BLOCKS, BLOCK), ((0, 128),), -0.2, 0.2)), 0.5, 2.0),
    }


smoothing = 1.0

def reference(velocity, z_inverse, tiles, amplitude, lateral, vertical, wall_velocity, surface):
    view = velocity.reshape(3, XW, NY // TY, TY, N_ROW, TZ).transpose(4, 1, 2, 0, 3, 5)
    block_rows = (jnp.arange(BLOCKS, dtype=jnp.int32) // (BLK_DEV * N_COL))[:, None]
    holder = tiles // T_DEV
    within = tiles % T_DEV
    plane = within // YTD
    band = holder * YTD + within % YTD
    picked = view[block_rows, plane, band]
    inner = jnp.einsum('bkcyz,bzi->bkcyi', picked, vertical, precision=lax.Precision.HIGHEST)
    weight = amplitude[:, :, None, :] * lateral[:, None, :, :]
    sampled = lax.optimization_barrier(jnp.sum(weight[:, :, None] * inner, axis=(1, 3)))
    marker_force = wall_velocity - sampled
    share = weight[:, :, None] * (surface[:, None, :] * marker_force)[:, None, :, None, :]
    spread = jnp.einsum('bkcyi,bzi->bkcyz', share, vertical, precision=lax.Precision.HIGHEST)
    forced_view = view.at[block_rows, plane, band].add(spread)
    forced = forced_view.transpose(3, 1, 2, 4, 0, 5).reshape(3, XW, NY, NZ)
    wave = jnp.arange(NY // 2).astype(jnp.float32)
    damping = 1.0 / (1.0 + 4.0 * smoothing * jnp.sin(jnp.pi * wave / NY) ** 2) / jnp.sqrt(jnp.float32(NY))

    def one_component(field):
        solved = jnp.einsum('xyz,zw->xyw', field, z_inverse, precision=lax.Precision.HIGHEST)
        modes = jnp.fft.rfft(solved, axis=1)[:, :NY // 2, :]
        scaled = modes * damping[None, :, None]
        return jnp.stack([jnp.real(scaled), jnp.imag(scaled)]).transpose(0, 1, 3, 2)
    spectra = lax.map(one_component, forced)
    spectrum = spectra.transpose(1, 0, 2, 3, 4)
    return (spectrum, marker_force)
```

```python
import functools
import numpy as np
import jax
import jax.numpy as jnp
from jax import lax
from jax.experimental import pallas as pl
from jax.experimental.pallas import tpu as pltpu
from jax.sharding import PartitionSpec as P

NY = 2048
TY = 8
K = 4
CAP = 8
TILES = 512
ROWS = 8
COLS = 16
SLOTS = COLS * CAP
REQ = 32
CHUNKS = 6

smoothing = 1.0

MESH = pl.DeviceIdType.MESH
F32 = jnp.float32
BF16 = jnp.bfloat16


def split(x):
    hi = x.astype(BF16)
    lo = (x - hi.astype(F32)).astype(BF16)
    return hi, lo


def dot(a, b, dims=((1,), (0,))):
    return lax.dot_general(a, b, (dims, ((), ())), preferred_element_type=F32)


def tables():
    k1 = np.arange(256)
    y2 = np.arange(256)
    phase = 2.0 * np.pi * ((k1[:, None] * y2[None, :]) % 256) / 256.0
    table = np.concatenate([np.cos(phase), -np.sin(phase)], axis=0).astype(np.float32)
    y1 = np.arange(8)
    turn = 2.0 * np.pi * (k1[:, None] * y1[None, :]) / NY
    twiddle = np.zeros((256, 128), np.float32)
    twiddle[:, 0:8] = np.cos(turn)
    twiddle[:, 8:16] = np.sin(turn)
    wave = np.arange(NY // 2, dtype=np.float64)
    damping = 1.0 / (1.0 + 4.0 * smoothing * np.sin(np.pi * wave / NY) ** 2) / np.sqrt(NY)
    return table, twiddle, damping.astype(np.float32)[None, :]


def kernel(
    vel, zinv, wanted, take_at, give_at, amp, lat, vert, wall, surf, table, tw_in, damp,
    out, force_out,
    v, zf, zh, zl, vth, vtl, weight, tab_h, tab_l, tw, ids, pick, put, take, give,
    fo, fr, spread, ro, ri, g, xh, s, h, u, xk, ob,
    load_sem, id_send, id_recv, f_send, f_recv, b_send, b_recv,
    r_send, r_recv, c_send, c_recv, o_sem,
):
    row = lax.axis_index("row")
    col = lax.axis_index("col")
    x = row // 2
    core = lax.rem(row, 2)
    z = col // 4
    y = lax.rem(col, 4)

    def row_peer(d):
        return lax.rem(x + d // 2, 4) * 2 + lax.rem(core + lax.rem(d, 2), 2)

    def col_peer(d):
        return lax.rem(z + d // 4, 4) * 4 + lax.rem(y + lax.rem(d, 4), 4)

    def rows(i, n):
        return pl.ds(pl.multiple_of(i * n, n), n)

    vel_copy = pltpu.make_async_copy(vel, v, load_sem.at[0])
    vel_copy.start()
    zinv_copy = pltpu.make_async_copy(zinv, zf, load_sem.at[1])
    zinv_copy.start()

    barrier = pltpu.get_barrier_semaphore()

    def greet_row(d, _):
        pl.semaphore_signal(barrier, 1, device_id={"row": row_peer(d)}, device_id_type=MESH)
        return 0

    def greet_col(d, _):
        pl.semaphore_signal(barrier, 1, device_id={"col": col_peer(d)}, device_id_type=MESH)
        return 0

    lax.fori_loop(1, COLS, greet_col, 0)
    lax.fori_loop(1, ROWS, greet_row, 0)

    def prepare(b, _):
        hi, lo = split(vert[b])
        vth[b] = hi
        vtl[b] = lo
        for k in range(K):
            weight[b, k * TY : (k + 1) * TY, :] = amp[b, k : k + 1, :] * lat[b]
        return 0

    lax.fori_loop(0, 8, prepare, 0)

    pl.semaphore_wait(barrier, ROWS + COLS - 2)

    def id_copy(peer):
        return pltpu.make_async_remote_copy(
            wanted.at[peer], ids.at[col], id_send.at[peer], id_recv.at[col],
            device_id={"col": peer}, device_id_type=MESH,
        )

    def id_wait(peer):
        pltpu.make_async_remote_copy(
            wanted.at[peer], ids.at[peer], id_send.at[peer], id_recv.at[peer],
            device_id={"col": peer}, device_id_type=MESH,
        ).wait_recv()

    def f_copy(c, peer):
        return pltpu.make_async_remote_copy(
            fo.at[c, rows(peer, 64)], fr.at[c, rows(col, 64)], f_send.at[c, peer], f_recv.at[c, col],
            device_id={"col": peer}, device_id_type=MESH,
        )

    def f_wait(c, peer):
        pltpu.make_async_remote_copy(
            fo.at[c, rows(peer, 64)], fr.at[c, rows(peer, 64)], f_send.at[c, peer], f_recv.at[c, peer],
            device_id={"col": peer}, device_id_type=MESH,
        ).wait_recv()

    def b_copy(c, peer):
        return pltpu.make_async_remote_copy(
            ro.at[c, rows(peer, 64)], ri.at[c, rows(col, 64)], b_send.at[c, peer], b_recv.at[c, col],
            device_id={"col": peer}, device_id_type=MESH,
        )

    def b_wait(c, peer):
        pltpu.make_async_remote_copy(
            ro.at[c, rows(peer, 64)], ri.at[c, rows(peer, 64)], b_send.at[c, peer], b_recv.at[c, peer],
            device_id={"col": peer}, device_id_type=MESH,
        ).wait_recv()

    def r_rows(n, peer):
        return pl.ds(pl.multiple_of((peer * 4 + 2 * lax.rem(n, 2)) * 128, 256), 256)

    def r_copy(n, peer):
        return pltpu.make_async_remote_copy(
            v.at[n // 2, r_rows(n, peer)], g.at[n, row], r_send.at[n, peer], r_recv.at[n, row],
            device_id={"row": peer}, device_id_type=MESH,
        )

    def r_wait(n, peer):
        pltpu.make_async_remote_copy(
            v.at[n // 2, r_rows(n, peer)], g.at[n, peer], r_send.at[n, peer], r_recv.at[n, peer],
            device_id={"row": peer}, device_id_type=MESH,
        ).wait_recv()

    def c_copy(n, peer):
        return pltpu.make_async_remote_copy(
            s.at[n, rows(peer, 128)], h.at[n, rows(col, 128)], c_send.at[n, peer], c_recv.at[n, col],
            device_id={"col": peer}, device_id_type=MESH,
        )

    def c_wait(n, peer):
        pltpu.make_async_remote_copy(
            s.at[n, rows(peer, 128)], h.at[n, rows(peer, 128)], c_send.at[n, peer], c_recv.at[n, peer],
            device_id={"col": peer}, device_id_type=MESH,
        ).wait_recv()

    def each_col(do):
        def step(d, _):
            do(col_peer(d))
            return 0

        lax.fori_loop(1, COLS, step, 0)

    def each_row(do):
        def step(d, _):
            do(row_peer(d))
            return 0

        lax.fori_loop(1, ROWS, step, 0)

    each_col(lambda p: id_copy(p).start())
    ids[col] = wanted[col]
    vel_copy.wait()
    each_col(id_wait)
    id_all = ids[...].reshape(SLOTS, 128)
    lane = lax.broadcasted_iota(jnp.int32, (128, 128), 1)
    for j in range(4):
        hit = jnp.where(id_all == lane + 128 * j, 1.0, 0.0).astype(F32)
        at = slice(j * 128, (j + 1) * 128)
        pick[:, at] = hit.astype(BF16)
        hit = hit.T.astype(BF16)
        put[at, 0:128] = hit
        put[at, 128:256] = hit

    def pair(ref, c, q, n):
        a = ref[c, pl.ds(2 * q, n, stride=TY), :]
        b = ref[c, pl.ds(2 * q + 1, n, stride=TY), :]
        return split(jnp.concatenate([a, b], axis=1))

    def gather(c):
        for q in range(4):
            hi, lo = pair(v, c, q, TILES)
            got = dot(pick[...], hi) + dot(pick[...], lo)
            for e in range(2):
                fo[c, pl.ds(2 * q + e, SLOTS, stride=TY), :] = got[:, e * 128 : (e + 1) * 128]
        each_col(lambda p: f_copy(c, p).start())
        fr[c, rows(col, 64), :] = fo[c, rows(col, 64), :]

    gather(0)
    gather(1)

    def select(at_ref, to, count, width):
        def block(i, _):
            at = rows(i, 128)
            for j in range(width // 128):
                hit = jnp.where(at_ref[at, :] == lane + 128 * j, 1.0, 0.0)
                to[at, j * 128 : (j + 1) * 128] = hit.astype(BF16)
            return 0

        lax.fori_loop(0, count // 128, block, 0)

    select(take_at, take, REQ * TY, SLOTS * TY)
    select(give_at, give, SLOTS * TY, REQ * TY)

    hi, lo = split(table[...])
    tab_h[...] = hi
    tab_l[...] = lo
    for i in range(16):
        tw[i] = jnp.broadcast_to(tw_in[:, i : i + 1], (256, 128))

    zinv_copy.wait()

    def cut(i, _):
        at = rows(i, 128)
        for j in range(4):
            hi, lo = split(zf[at, j * 256 : (j + 1) * 256])
            zh[j, at, :] = hi
            zl[j, at, :] = lo
        return 0

    lax.fori_loop(0, 8, cut, 0)

    def markers(c):
        each_col(lambda p: f_wait(c, p))
        f_hi, f_lo = split(fr[c])
        mine = dot(take[...], f_hi) + dot(take[...], f_lo)
        for b in range(8):
            at = slice(b * K * TY, (b + 1) * K * TY)
            p_hi, p_lo = split(mine[at, :])
            inner = dot(p_hi, vth[b]) + (dot(p_lo, vth[b]) + dot(p_hi, vtl[b]))
            w = weight[b]
            sampled = jnp.sum(w * inner, axis=0, keepdims=True)
            force = wall[c, b : b + 1, :] - sampled
            force_out[c, b : b + 1, :] = force
            s_hi, s_lo = split(w * (surf[b : b + 1, :] * force))
            last = ((1,), (1,))
            back = dot(s_hi, vth[b], last) + (dot(s_lo, vth[b], last) + dot(s_hi, vtl[b], last))
            spread[at, :] = back
        b_hi, b_lo = split(spread[...])
        ro[c] = dot(give[...], b_hi) + dot(give[...], b_lo)
        each_col(lambda p: b_copy(c, p).start())
        ri[c, rows(col, 64), :] = ro[c, rows(col, 64), :]

    def force_tiles(c):
        each_col(lambda p: b_wait(c, p))
        for q in range(4):
            hi, lo = pair(ri, c, q, SLOTS)
            delta = dot(put[...], jnp.concatenate([hi, lo], axis=0))
            for e in range(2):
                at = pl.ds(2 * q + e, TILES, stride=TY)
                v[c, at, :] = v[c, at, :] + delta[:, e * 128 : (e + 1) * 128]
        for e in range(2):
            n = 2 * c + e
            each_row(lambda p: r_copy(n, p).start())
            g[n, row] = v[c, r_rows(n, row), :]

    def first(c, _):
        @pl.when(c < 3)
        def _():
            markers(c)

        @pl.when(c == 0)
        def _():
            gather(2)

        @pl.when(c > 0)
        def _():
            force_tiles(c - 1)

        return 0

    lax.fori_loop(0, 4, first, 0)

    low = lane < 64

    def axial(n):
        each_row(lambda p: r_wait(n, p))
        for r in range(ROWS):
            hi, lo = split(g[n, r])
            xh[0:256, r * 128 : (r + 1) * 128] = hi
            xh[256:512, r * 128 : (r + 1) * 128] = lo

        def tile(j, _):
            acc = dot(xh[...], zh[j])
            acc = acc[0:256] + (acc[256:512] + dot(xh[0:256, :], zl[j]))
            for t in range(2):
                a0 = acc[0:128, t * 128 : (t + 1) * 128]
                a1 = acc[128:256, t * 128 : (t + 1) * 128]
                s[n, rows(4 * j + 2 * t, 128), :] = jnp.where(low, a0, pltpu.roll(a1, 64, 1))
                s[n, rows(4 * j + 2 * t + 1, 128), :] = jnp.where(low, pltpu.roll(a0, 64, 1), a1)
            return 0

        lax.fori_loop(0, 4, tile, 0)
        each_col(lambda p: c_copy(n, p).start())
        h[n, rows(col, 128), :] = s[n, rows(col, 128), :]

    def out_copy(n):
        return pltpu.make_async_copy(ob.at[n], out.at[:, n // 2, lax.rem(n, 2)], o_sem.at[n])

    half = np.float32(np.sqrt(0.5))

    def fourier(n):
        each_col(lambda p: c_wait(n, p))
        for q in range(4):
            a = h[n, pl.ds(2 * q, 256, stride=8), :]
            b = h[n, pl.ds(2 * q + 1, 256, stride=8), :]
            hi, lo = split(jnp.concatenate([a, b], axis=1))
            acc = dot(tab_h[...], hi) + (dot(tab_h[...], lo) + dot(tab_l[...], hi))
            u[2 * q] = acc[:, 0:128]
            u[2 * q + 1] = acc[:, 128:256]

        def combine(i, _):
            re = rows(i, 8)
            im = pl.ds(pl.multiple_of(256 + i * 8, 8), 8)
            a = []
            for m in range(8):
                ur, ui = u[m, re, :], u[m, im, :]
                if m > 0:
                    tc, ts = tw[m, re, :], tw[8 + m, re, :]
                    ur, ui = ur * tc + ui * ts, ui * tc - ur * ts
                a.append((ur, ui))

            def add(p, q):
                return (p[0] + q[0], p[1] + q[1])

            def sub(p, q):
                return (p[0] - q[0], p[1] - q[1])

            def turn(p):
                return (p[1], -p[0])

            def four(p, q, r, t):
                s0, d0, s1, d1 = add(p, r), sub(p, r), add(q, t), turn(sub(q, t))
                return add(s0, s1), add(d0, d1), sub(s0, s1), sub(d0, d1)

            e0, e1, e2, e3 = four(a[0], a[2], a[4], a[6])
            o0, o1, o2, o3 = four(a[1], a[3], a[5], a[7])
            o1 = ((o1[0] + o1[1]) * half, (o1[1] - o1[0]) * half)
            o3 = ((o3[1] - o3[0]) * half, (-o3[1] - o3[0]) * half)
            for k2, (e, o) in enumerate(((e0, o0), (e1, o1), (e2, turn(o2)), (e3, o3))):
                xr, xi = add(e, o)
                xk[0, k2, re, :] = xr
                xk[1, k2, re, :] = xi
            return 0

        lax.fori_loop(0, 32, combine, 0, unroll=2)
        for p in range(2):
            for k2 in range(4):
                at = slice(k2 * 256, (k2 + 1) * 256)
                ob[n, p, :, at] = xk[p, k2].T * damp[:, at]
        out_copy(n).start()

    def second(n, _):
        @pl.when(n < CHUNKS)
        def _():
            axial(n)

        @pl.when(n > 0)
        def _():
            fourier(n - 1)

        return 0

    lax.fori_loop(0, CHUNKS + 1, second, 0)

    each_col(lambda p: id_copy(p).wait_send())

    def drain3(c, _):
        each_col(lambda p: f_copy(c, p).wait_send())
        each_col(lambda p: b_copy(c, p).wait_send())
        return 0

    def drain6(n, _):
        each_row(lambda p: r_copy(n, p).wait_send())
        each_col(lambda p: c_copy(n, p).wait_send())
        out_copy(n).wait()
        return 0

    lax.fori_loop(0, 3, drain3, 0)
    lax.fori_loop(0, CHUNKS, drain6, 0)


def local(velocity, z_inverse, tiles, amplitude, lateral, vertical, wall_velocity, surface):
    wants = tiles.reshape(-1)
    holder = wants // TILES
    within = wants % TILES
    order = jnp.arange(REQ, dtype=jnp.int32)
    before = (holder[:, None] == holder[None, :]) & (order[None, :] < order[:, None])
    slot_of = holder * CAP + jnp.sum(before.astype(jnp.int32), axis=1)
    match = jnp.arange(SLOTS, dtype=jnp.int32)[:, None] == slot_of[None, :]
    wanted = jnp.sum(jnp.where(match, within[None, :], 0), axis=1)
    source = jnp.sum(jnp.where(match, order[None, :] - REQ, 0), axis=1) + REQ
    wanted = jnp.broadcast_to(wanted[:, None], (SLOTS, 128)).reshape(COLS, CAP, 128)
    line = jnp.arange(TY, dtype=jnp.int32)

    def spread_out(index):
        cells = index[:, None, None] * TY + line[None, :, None]
        return jnp.broadcast_to(cells, (index.shape[0], TY, 128)).reshape(-1, 128)

    table, twiddle, damping = tables()
    any_ = pl.BlockSpec(memory_space=pl.ANY)
    vmem = pl.BlockSpec(memory_space=pltpu.VMEM)
    dma = pltpu.SemaphoreType.DMA
    spectrum, force = pl.pallas_call(
        kernel,
        out_shape=(
            jax.ShapeDtypeStruct((2, 3, 2, 128, 1024), F32),
            jax.ShapeDtypeStruct((3, 8, 256), F32),
        ),
        in_specs=[any_, any_] + [vmem] * 11,
        out_specs=(any_, vmem),
        scratch_shapes=[
            pltpu.VMEM((3, 4096, 128), F32),
            pltpu.VMEM((1024, 1024), F32),
            pltpu.VMEM((4, 1024, 256), BF16),
            pltpu.VMEM((4, 1024, 256), BF16),
            pltpu.VMEM((8, 128, 256), BF16),
            pltpu.VMEM((8, 128, 256), BF16),
            pltpu.VMEM((8, 32, 256), F32),
            pltpu.VMEM((512, 256), BF16),
            pltpu.VMEM((512, 256), BF16),
            pltpu.VMEM((16, 256, 128), F32),
            pltpu.VMEM((COLS, CAP, 128), jnp.int32),
            pltpu.VMEM((SLOTS, TILES), BF16),
            pltpu.VMEM((TILES, 2 * SLOTS), BF16),
            pltpu.VMEM((REQ * TY, SLOTS * TY), BF16),
            pltpu.VMEM((SLOTS * TY, REQ * TY), BF16),
            pltpu.VMEM((3, SLOTS * TY, 128), F32),
            pltpu.VMEM((3, SLOTS * TY, 128), F32),
            pltpu.VMEM((REQ * TY, 128), F32),
            pltpu.VMEM((3, SLOTS * TY, 128), F32),
            pltpu.VMEM((3, SLOTS * TY, 128), F32),
            pltpu.VMEM((CHUNKS, ROWS, 256, 128), F32),
            pltpu.VMEM((512, 1024), BF16),
            pltpu.VMEM((CHUNKS, NY, 128), F32),
            pltpu.VMEM((CHUNKS, NY, 128), F32),
            pltpu.VMEM((8, 512, 128), F32),
            pltpu.VMEM((2, 4, 256, 128), F32),
            pltpu.VMEM((CHUNKS, 2, 128, 1024), F32),
            dma((2,)),
            dma((COLS,)), dma((COLS,)),
            dma((3, COLS)), dma((3, COLS)),
            dma((3, COLS)), dma((3, COLS)),
            dma((CHUNKS, ROWS)), dma((CHUNKS, ROWS)),
            dma((CHUNKS, COLS)), dma((CHUNKS, COLS)),
            dma((CHUNKS,)),
        ],
        compiler_params=pltpu.CompilerParams(
            collective_id=0, has_side_effects=True, vmem_limit_bytes=60 * 1024 * 1024
        ),
        name="slab",
    )(
        velocity.reshape(3, 4096, 128), z_inverse, wanted, spread_out(slot_of), spread_out(source),
        amplitude, lateral, vertical, wall_velocity.transpose(1, 0, 2), surface,
        jnp.asarray(table), jnp.asarray(twiddle), jnp.asarray(damping),
    )
    return (spectrum.reshape(2, 3, 4, 64, 1024), force.transpose(1, 0, 2))


def solution(mesh):
    in_specs = (
        P(None, None, "col", "row"),
        P(),
        P(("row", "col"), None),
        P(("row", "col"), None, None),
        P(("row", "col"), None, None),
        P(("row", "col"), None, None),
        P(("row", "col"), None, None),
        P(("row", "col"), None),
    )
    out_specs = (P(None, None, "row", "col", None), P(("row", "col"), None, None))
    return jax.shard_map(local, mesh=mesh, in_specs=in_specs, out_specs=out_specs, check_vma=False)
```

```python
import functools
import numpy as np
import jax
import jax.numpy as jnp
from jax import lax
from jax.experimental import pallas as pl
from jax.experimental.pallas import tpu as pltpu
from jax.sharding import PartitionSpec as P

NY = 2048
TY = 8
K = 4
CAP = 8
TILES = 512
ROWS = 8
COLS = 16
SLOTS = COLS * CAP
REQ = 32
CHUNKS = 6

smoothing = 1.0

MESH = pl.DeviceIdType.MESH
F32 = jnp.float32
BF16 = jnp.bfloat16


def split(x):
    hi = x.astype(BF16)
    lo = (x - hi.astype(F32)).astype(BF16)
    return hi, lo


def dot(a, b, dims=((1,), (0,))):
    return lax.dot_general(a, b, (dims, ((), ())), preferred_element_type=F32)


def tables():
    k1 = np.arange(256)
    y2 = np.arange(256)
    phase = 2.0 * np.pi * ((k1[:, None] * y2[None, :]) % 256) / 256.0
    table = np.concatenate([np.cos(phase), -np.sin(phase)], axis=0).astype(np.float32)
    y1 = np.arange(8)
    turn = 2.0 * np.pi * (k1[:, None] * y1[None, :]) / NY
    twiddle = np.zeros((256, 128), np.float32)
    twiddle[:, 0:8] = np.cos(turn)
    twiddle[:, 8:16] = np.sin(turn)
    wave = np.arange(NY // 2, dtype=np.float64)
    damping = 1.0 / (1.0 + 4.0 * smoothing * np.sin(np.pi * wave / NY) ** 2) / np.sqrt(NY)
    return table, twiddle, damping.astype(np.float32)[None, :]


def kernel(
    vel, zinv, tiles_in, amp_in, lat_in, vert_in, wall_in, surf_in, table_in, tw_hbm, damp_in,
    out, force_out,
    tiles, amp, lat, vert, wall, surf, table, tw_in, damp, wanted,
    v, zf, zh, zl, vth, vtl, weight, tab_h, tab_l, tw, ids, pick, put, take, give,
    fo, fr, spread, ro, ri, g, xh, s, h, u, xk, ob,
    load_sem, id_send, id_recv, f_send, f_recv, b_send, b_recv,
    r_send, r_recv, c_send, c_recv, o_sem,
):
    row = lax.axis_index("row")
    col = lax.axis_index("col")
    x = row // 2
    core = lax.rem(row, 2)
    z = col // 4
    y = lax.rem(col, 4)

    def row_peer(d):
        return lax.rem(x + d // 2, 4) * 2 + lax.rem(core + lax.rem(d, 2), 2)

    def col_peer(d):
        return lax.rem(z + d // 4, 4) * 4 + lax.rem(y + lax.rem(d, 4), 4)

    def rows(i, n):
        return pl.ds(pl.multiple_of(i * n, n), n)

    barrier = pltpu.get_barrier_semaphore()

    def greet_row(d, _):
        pl.semaphore_signal(barrier, 1, device_id={"row": row_peer(d)}, device_id_type=MESH)
        return 0

    def greet_col(d, _):
        pl.semaphore_signal(barrier, 1, device_id={"col": col_peer(d)}, device_id_type=MESH)
        return 0

    lax.fori_loop(1, COLS, greet_col, 0)
    lax.fori_loop(1, ROWS, greet_row, 0)

    pairs = (
        (tiles_in, tiles), (vert_in, vert), (amp_in, amp), (lat_in, lat), (vel, v), (zinv, zf),
        (wall_in, wall), (surf_in, surf), (table_in, table), (tw_hbm, tw_in), (damp_in, damp),
    )
    loads = [pltpu.make_async_copy(a, b, load_sem.at[i]) for i, (a, b) in enumerate(pairs)]
    for load in loads:
        load.start()

    loads[0].wait()
    wants = [tiles[n // 8, n % 8] for n in range(REQ)]
    holders = [lax.shift_right_logical(w, 9) for w in wants]
    slots = []
    for n in range(REQ):
        rank = 0
        for m in range(n):
            rank = rank + (holders[m] == holders[n]).astype(jnp.int32)
        slots.append(holders[n] * CAP + rank)
    lane = lax.broadcasted_iota(jnp.int32, (128, 128), 1)
    place = lax.broadcasted_iota(jnp.int32, (SLOTS, 128), 0)
    named = jnp.zeros((SLOTS, 128), jnp.int32)
    for n in range(REQ):
        named = jnp.where(place == slots[n], wants[n] - holders[n] * TILES, named)
    wanted[...] = named.reshape(COLS, CAP, 128)

    pl.semaphore_wait(barrier, ROWS + COLS - 2)

    east = col_peer(1)
    north = row_peer(2)

    def to_col(a, b, sems, peer):
        return pltpu.make_async_remote_copy(
            a, b, sems[0], sems[1], device_id={"col": peer}, device_id_type=MESH
        )

    def to_row(a, b, sems, peer):
        return pltpu.make_async_remote_copy(
            a, b, sems[0], sems[1], device_id={"row": peer}, device_id_type=MESH
        )

    id_sems = (id_send.at[0], id_recv.at[0])

    def id_copy(peer):
        return to_col(wanted.at[peer], ids.at[col], id_sems, peer)

    def id_all_copies():
        rest = pl.ds(0, COLS - 1)
        return to_col(wanted.at[rest], ids.at[rest], id_sems, east)

    many = pl.ds(0, (COLS - 1) * 64)

    def f_copy(c, peer):
        sems = (f_send.at[c], f_recv.at[c])
        return to_col(fo.at[c, rows(peer, 64)], fr.at[c, rows(col, 64)], sems, peer)

    def f_all(c):
        return to_col(fo.at[c, many], fr.at[c, many], (f_send.at[c], f_recv.at[c]), east)

    def b_copy(c, peer):
        sems = (b_send.at[c], b_recv.at[c])
        return to_col(ro.at[c, rows(peer, 64)], ri.at[c, rows(col, 64)], sems, peer)

    def b_all(c):
        return to_col(ro.at[c, many], ri.at[c, many], (b_send.at[c], b_recv.at[c]), east)

    def r_rows(n, peer):
        return pl.ds(pl.multiple_of((peer * 4 + 2 * lax.rem(n, 2)) * 128, 256), 256)

    def r_copy(n, peer):
        sems = (r_send.at[n], r_recv.at[n])
        return to_row(v.at[n // 2, r_rows(n, peer)], g.at[n, rows(row, 256)], sems, peer)

    def r_all(n):
        most = pl.ds(0, (ROWS - 1) * 256)
        return to_row(v.at[n // 2, most], g.at[n, most], (r_send.at[n], r_recv.at[n]), north)

    def c_copy(n, peer):
        sems = (c_send.at[n], c_recv.at[n])
        return to_col(s.at[n, rows(peer, 128)], h.at[n, rows(col, 128)], sems, peer)

    def c_all(n):
        most = pl.ds(0, (COLS - 1) * 128)
        return to_col(s.at[n, most], h.at[n, most], (c_send.at[n], c_recv.at[n]), east)

    def each_col(do):
        def step(d, _):
            do(col_peer(d))
            return 0

        lax.fori_loop(1, COLS, step, 0)

    def each_row(do):
        def step(d, _):
            do(row_peer(d))
            return 0

        lax.fori_loop(1, ROWS, step, 0)

    each_col(lambda p: id_copy(p).start())
    ids[col] = wanted[col]

    for load in loads[1:4] + loads[8:10]:
        load.wait()
    def prepare(b, _):
        hi, lo = split(vert[b])
        vth[b] = hi
        vtl[b] = lo
        for k in range(K):
            weight[b, k * TY : (k + 1) * TY, :] = amp[b, k : k + 1, :] * lat[b]
        return 0

    lax.fori_loop(0, 8, prepare, 0)

    wide = lax.broadcasted_iota(jnp.int32, (2 * TY, SLOTS * TY), 1)
    deep = lax.broadcasted_iota(jnp.int32, (2 * TY, SLOTS * TY), 0)
    for n in range(0, REQ, 2):
        cell = jnp.where(deep < TY, slots[n] * TY + deep, slots[n + 1] * TY + deep - TY)
        take[n * TY : (n + 2) * TY, :] = jnp.where(wide == cell, 1.0, 0.0).astype(BF16)
    across = lax.broadcasted_iota(jnp.int32, (8, REQ * TY), 1)
    cell = jnp.zeros((8, REQ * TY), jnp.int32)
    for n in range(REQ):
        cell = jnp.where(lax.shift_right_logical(across, 3) == n, slots[n] * TY, cell)
    cell = jnp.broadcast_to((cell + (across & 7))[0:1], (128, REQ * TY))
    down = lax.broadcasted_iota(jnp.int32, (128, REQ * TY), 0)

    def build(i, _):
        give[rows(i, 128), :] = jnp.where(down + i * 128 == cell, 1.0, 0.0).astype(BF16)
        return 0

    lax.fori_loop(0, SLOTS * TY // 128, build, 0)

    hi, lo = split(table[...])
    tab_h[...] = hi
    tab_l[...] = lo
    for i in range(16):
        tw[i] = jnp.broadcast_to(tw_in[:, i : i + 1], (256, 128))

    loads[4].wait()
    id_all_copies().wait_recv()
    id_all = ids[...].reshape(SLOTS, 128)
    for j in range(4):
        hit = jnp.where(id_all == lane + 128 * j, 1.0, 0.0).astype(F32)
        at = slice(j * 128, (j + 1) * 128)
        pick[:, at] = hit.astype(BF16)
        hit = hit.T.astype(BF16)
        put[at, 0:128] = hit
        put[at, 128:256] = hit

    def pair(ref, c, q, n):
        a = ref[c, pl.ds(2 * q, n, stride=TY), :]
        b = ref[c, pl.ds(2 * q + 1, n, stride=TY), :]
        return split(jnp.concatenate([a, b], axis=1))

    def gather(c):
        for q in range(4):
            hi, lo = pair(v, c, q, TILES)
            got = dot(pick[...], hi) + dot(pick[...], lo)
            for e in range(2):
                fo[c, pl.ds(2 * q + e, SLOTS, stride=TY), :] = got[:, e * 128 : (e + 1) * 128]
        each_col(lambda p: f_copy(c, p).start())
        fr[c, rows(col, 64), :] = fo[c, rows(col, 64), :]

    gather(0)
    gather(1)

    for load in loads[5:8] + loads[10:]:
        load.wait()

    def cut(i, _):
        at = rows(i, 128)
        for j in range(4):
            hi, lo = split(zf[at, j * 256 : (j + 1) * 256])
            zh[j, at, :] = hi
            zl[j, at, :] = lo
        return 0

    lax.fori_loop(0, 8, cut, 0)

    def markers(c):
        f_all(c).wait_recv()
        f_hi, f_lo = split(fr[c])
        mine = dot(take[...], f_hi) + dot(take[...], f_lo)
        for b in range(8):
            own = [slice((k * 8 + b) * TY, (k * 8 + b + 1) * TY) for k in range(K)]
            p_hi, p_lo = split(jnp.concatenate([mine[at, :] for at in own], axis=0))
            inner = dot(p_hi, vth[b]) + (dot(p_lo, vth[b]) + dot(p_hi, vtl[b]))
            w = weight[b]
            sampled = jnp.sum(w * inner, axis=0, keepdims=True)
            force = wall[c, b : b + 1, :] - sampled
            force_out[c, b : b + 1, :] = force
            s_hi, s_lo = split(w * (surf[b : b + 1, :] * force))
            last = ((1,), (1,))
            back = dot(s_hi, vth[b], last) + (dot(s_lo, vth[b], last) + dot(s_hi, vtl[b], last))
            for k in range(K):
                spread[own[k], :] = back[k * TY : (k + 1) * TY, :]
        b_hi, b_lo = split(spread[...])
        ro[c] = dot(give[...], b_hi) + dot(give[...], b_lo)
        each_col(lambda p: b_copy(c, p).start())
        ri[c, rows(col, 64), :] = ro[c, rows(col, 64), :]

    def row_sends(n):
        each_row(lambda p: r_copy(n, p).start())
        g[n, rows(row, 256), :] = v[n // 2, r_rows(n, row), :]

    def force_tiles(c):
        b_all(c).wait_recv()
        for q in range(4):
            hi, lo = pair(ri, c, q, SLOTS)
            delta = dot(put[...], jnp.concatenate([hi, lo], axis=0))
            for e in range(2):
                at = pl.ds(2 * q + e, TILES, stride=TY)
                v[c, at, :] = v[c, at, :] + delta[:, e * 128 : (e + 1) * 128]
        row_sends(c)

    def first(c, _):
        @pl.when(c < 3)
        def _():
            markers(c)

        @pl.when(c == 0)
        def _():
            gather(2)

        @pl.when(c > 0)
        def _():
            force_tiles(c - 1)

        return 0

    lax.fori_loop(0, 4, first, 0)

    low = lane < 64

    def axial(n):
        r_all(n).wait_recv()

        @pl.when(n < 3)
        def _():
            row_sends(n + 3)

        for r in range(ROWS):
            hi, lo = split(g[n, r * 256 : (r + 1) * 256, :])
            xh[0:256, r * 128 : (r + 1) * 128] = hi
            xh[256:512, r * 128 : (r + 1) * 128] = lo

        def tile(j, _):
            acc = dot(xh[...], zh[j])
            acc = acc[0:256] + (acc[256:512] + dot(xh[0:256, :], zl[j]))
            for t in range(2):
                a0 = acc[0:128, t * 128 : (t + 1) * 128]
                a1 = acc[128:256, t * 128 : (t + 1) * 128]
                s[n, rows(4 * j + 2 * t, 128), :] = jnp.where(low, a0, pltpu.roll(a1, 64, 1))
                s[n, rows(4 * j + 2 * t + 1, 128), :] = jnp.where(low, pltpu.roll(a0, 64, 1), a1)
            return 0

        lax.fori_loop(0, 4, tile, 0)
        each_col(lambda p: c_copy(n, p).start())
        h[n, rows(col, 128), :] = s[n, rows(col, 128), :]

    def out_copy(n):
        return pltpu.make_async_copy(ob.at[n], out.at[:, n // 2, lax.rem(n, 2)], o_sem.at[n])

    half = np.float32(np.sqrt(0.5))

    def fourier(n):
        c_all(n).wait_recv()
        for q in range(4):
            a = h[n, pl.ds(2 * q, 256, stride=8), :]
            b = h[n, pl.ds(2 * q + 1, 256, stride=8), :]
            hi, lo = split(jnp.concatenate([a, b], axis=1))
            acc = dot(tab_h[...], hi) + (dot(tab_h[...], lo) + dot(tab_l[...], hi))
            u[2 * q] = acc[:, 0:128]
            u[2 * q + 1] = acc[:, 128:256]

        def combine(i, _):
            re = rows(i, 8)
            im = pl.ds(pl.multiple_of(256 + i * 8, 8), 8)
            a = []
            for m in range(8):
                ur, ui = u[m, re, :], u[m, im, :]
                if m > 0:
                    tc, ts = tw[m, re, :], tw[8 + m, re, :]
                    ur, ui = ur * tc + ui * ts, ui * tc - ur * ts
                a.append((ur, ui))

            def add(p, q):
                return (p[0] + q[0], p[1] + q[1])

            def sub(p, q):
                return (p[0] - q[0], p[1] - q[1])

            def turn(p):
                return (p[1], -p[0])

            def four(p, q, r, t):
                s0, d0, s1, d1 = add(p, r), sub(p, r), add(q, t), turn(sub(q, t))
                return add(s0, s1), add(d0, d1), sub(s0, s1), sub(d0, d1)

            e0, e1, e2, e3 = four(a[0], a[2], a[4], a[6])
            o0, o1, o2, o3 = four(a[1], a[3], a[5], a[7])
            o1 = ((o1[0] + o1[1]) * half, (o1[1] - o1[0]) * half)
            o3 = ((o3[1] - o3[0]) * half, (-o3[1] - o3[0]) * half)
            for k2, (e, o) in enumerate(((e0, o0), (e1, o1), (e2, turn(o2)), (e3, o3))):
                xr, xi = add(e, o)
                xk[0, k2, re, :] = xr
                xk[1, k2, re, :] = xi
            return 0

        lax.fori_loop(0, 32, combine, 0, unroll=2)
        for p in range(2):
            for k2 in range(4):
                at = slice(k2 * 256, (k2 + 1) * 256)
                ob[n, p, :, at] = xk[p, k2].T * damp[:, at]
        out_copy(n).start()

    def second(n, _):
        @pl.when(n < CHUNKS)
        def _():
            axial(n)

        @pl.when(n > 0)
        def _():
            fourier(n - 1)

        return 0

    lax.fori_loop(0, CHUNKS + 1, second, 0)

    id_all_copies().wait_send()
    for c in range(3):
        f_all(c).wait_send()
        b_all(c).wait_send()
    for n in range(CHUNKS):
        r_all(n).wait_send()
        c_all(n).wait_send()
        out_copy(n).wait()


def local(velocity, z_inverse, tiles, amplitude, lateral, vertical, wall_velocity, surface):
    table, twiddle, damping = tables()
    any_ = pl.BlockSpec(memory_space=pl.ANY)
    vmem = pl.BlockSpec(memory_space=pltpu.VMEM)
    dma = pltpu.SemaphoreType.DMA
    spectrum, force = pl.pallas_call(
        kernel,
        out_shape=(
            jax.ShapeDtypeStruct((2, 3, 2, 128, 1024), F32),
            jax.ShapeDtypeStruct((3, 8, 256), F32),
        ),
        in_specs=[any_] * 11,
        out_specs=(any_, vmem),
        scratch_shapes=[
            pltpu.SMEM((4, 8), jnp.int32),
            pltpu.VMEM((8, 4, 256), F32),
            pltpu.VMEM((8, 8, 256), F32),
            pltpu.VMEM((8, 128, 256), F32),
            pltpu.VMEM((3, 8, 256), F32),
            pltpu.VMEM((8, 256), F32),
            pltpu.VMEM((512, 256), F32),
            pltpu.VMEM((256, 128), F32),
            pltpu.VMEM((1, 1024), F32),
            pltpu.VMEM((COLS, CAP, 128), jnp.int32),
            pltpu.VMEM((3, 4096, 128), F32),
            pltpu.VMEM((1024, 1024), F32),
            pltpu.VMEM((4, 1024, 256), BF16),
            pltpu.VMEM((4, 1024, 256), BF16),
            pltpu.VMEM((8, 128, 256), BF16),
            pltpu.VMEM((8, 128, 256), BF16),
            pltpu.VMEM((8, 32, 256), F32),
            pltpu.VMEM((512, 256), BF16),
            pltpu.VMEM((512, 256), BF16),
            pltpu.VMEM((16, 256, 128), F32),
            pltpu.VMEM((COLS, CAP, 128), jnp.int32),
            pltpu.VMEM((SLOTS, TILES), BF16),
            pltpu.VMEM((TILES, 2 * SLOTS), BF16),
            pltpu.VMEM((REQ * TY, SLOTS * TY), BF16),
            pltpu.VMEM((SLOTS * TY, REQ * TY), BF16),
            pltpu.VMEM((3, SLOTS * TY, 128), F32),
            pltpu.VMEM((3, SLOTS * TY, 128), F32),
            pltpu.VMEM((REQ * TY, 128), F32),
            pltpu.VMEM((3, SLOTS * TY, 128), F32),
            pltpu.VMEM((3, SLOTS * TY, 128), F32),
            pltpu.VMEM((CHUNKS, ROWS * 256, 128), F32),
            pltpu.VMEM((512, 1024), BF16),
            pltpu.VMEM((CHUNKS, NY, 128), F32),
            pltpu.VMEM((CHUNKS, NY, 128), F32),
            pltpu.VMEM((8, 512, 128), F32),
            pltpu.VMEM((2, 4, 256, 128), F32),
            pltpu.VMEM((CHUNKS, 2, 128, 1024), F32),
            dma((11,)), dma((1,)), dma((1,)),
            dma((3,)), dma((3,)), dma((3,)), dma((3,)),
            dma((CHUNKS,)), dma((CHUNKS,)), dma((CHUNKS,)), dma((CHUNKS,)), dma((CHUNKS,)),
        ],
        compiler_params=pltpu.CompilerParams(
            collective_id=0, has_side_effects=True, vmem_limit_bytes=60 * 1024 * 1024
        ),
        name="slab",
    )(
        velocity.reshape(3, 4096, 128), z_inverse, tiles.T, amplitude, lateral, vertical, wall_velocity.transpose(1, 0, 2), surface,
        jnp.asarray(table), jnp.asarray(twiddle), jnp.asarray(damping),
    )
    return (spectrum.reshape(2, 3, 4, 64, 1024), force.transpose(1, 0, 2))


def solution(mesh):
    in_specs = (
        P(None, None, "col", "row"),
        P(),
        P(("row", "col"), None),
        P(("row", "col"), None, None),
        P(("row", "col"), None, None),
        P(("row", "col"), None, None),
        P(("row", "col"), None, None),
        P(("row", "col"), None),
    )
    out_specs = (P(None, None, "row", "col", None), P(("row", "col"), None, None))
    return jax.shard_map(local, mesh=mesh, in_specs=in_specs, out_specs=out_specs, check_vma=False)
```

```python
import functools
import numpy as np
import jax
import jax.numpy as jnp
from jax import lax
from jax.experimental import pallas as pl
from jax.experimental.pallas import tpu as pltpu
from jax.sharding import PartitionSpec as P

NY = 2048
TY = 8
K = 4
CAP = 8
TILES = 512
ROWS = 8
COLS = 16
SLOTS = COLS * CAP
REQ = 32
CHUNKS = 6

smoothing = 1.0

MESH = pl.DeviceIdType.MESH
F32 = jnp.float32
BF16 = jnp.bfloat16


def split(x):
    hi = x.astype(BF16)
    lo = (x - hi.astype(F32)).astype(BF16)
    return hi, lo


def dot(a, b, dims=((1,), (0,))):
    return lax.dot_general(a, b, (dims, ((), ())), preferred_element_type=F32)


def tables():
    k1 = np.arange(256)
    y2 = np.arange(256)
    phase = 2.0 * np.pi * ((k1[:, None] * y2[None, :]) % 256) / 256.0
    table = np.concatenate([np.cos(phase), -np.sin(phase)], axis=0).astype(np.float32)
    y1 = np.arange(8)
    turn = 2.0 * np.pi * (k1[:, None] * y1[None, :]) / NY
    twiddle = np.zeros((256, 128), np.float32)
    twiddle[:, 0:8] = np.cos(turn)
    twiddle[:, 8:16] = np.sin(turn)
    wave = np.arange(NY // 2, dtype=np.float64)
    damping = 1.0 / (1.0 + 4.0 * smoothing * np.sin(np.pi * wave / NY) ** 2) / np.sqrt(NY)
    return table, twiddle, damping.astype(np.float32)[None, :]


def kernel(
    vel, zinv, tiles_in, amp_in, lat_in, vert_in, wall_in, surf_in, table_in, tw_hbm, damp_in,
    out, force_out,
    tiles, amp, lat, vert, wall, surf, table, tw_in, damp, wanted,
    v, zf, zh, zl, vth, vtl, weight, tab_h, tab_l, tw, ids, pick, put, take, give,
    fo, fr, spread, ro, ri, g, xh, s, h, u, xk,
    load_sem, id_send, id_recv, f_send, f_recv, b_send, b_recv,
    r_send, r_recv, c_send, c_recv,
):
    row = lax.axis_index("row")
    col = lax.axis_index("col")
    x = row // 2
    core = lax.rem(row, 2)
    z = col // 4
    y = lax.rem(col, 4)

    def row_peer(d):
        return lax.rem(x + d // 2, 4) * 2 + lax.rem(core + lax.rem(d, 2), 2)

    def col_peer(d):
        return lax.rem(z + d // 4, 4) * 4 + lax.rem(y + lax.rem(d, 4), 4)

    def rows(i, n):
        return pl.ds(pl.multiple_of(i * n, n), n)

    barrier = pltpu.get_barrier_semaphore()

    def greet_row(d, _):
        pl.semaphore_signal(barrier, 1, device_id={"row": row_peer(d)}, device_id_type=MESH)
        return 0

    def greet_col(d, _):
        pl.semaphore_signal(barrier, 1, device_id={"col": col_peer(d)}, device_id_type=MESH)
        return 0

    lax.fori_loop(1, COLS, greet_col, 0)
    lax.fori_loop(1, ROWS, greet_row, 0)

    pairs = (
        (tiles_in, tiles), (vert_in, vert), (amp_in, amp), (lat_in, lat), (vel, v), (zinv, zf),
        (wall_in, wall), (surf_in, surf), (table_in, table), (tw_hbm, tw_in), (damp_in, damp),
    )
    loads = [pltpu.make_async_copy(a, b, load_sem.at[i]) for i, (a, b) in enumerate(pairs)]
    for load in loads:
        load.start()

    loads[0].wait()
    wants = [tiles[n // 8, n % 8] for n in range(REQ)]
    holders = [lax.shift_right_logical(w, 9) for w in wants]
    slots = []
    for n in range(REQ):
        rank = 0
        for m in range(n):
            rank = rank + (holders[m] == holders[n]).astype(jnp.int32)
        slots.append(holders[n] * CAP + rank)
    lane = lax.broadcasted_iota(jnp.int32, (128, 128), 1)
    place = lax.broadcasted_iota(jnp.int32, (SLOTS, 128), 0)
    named = jnp.zeros((SLOTS, 128), jnp.int32)
    for n in range(REQ):
        named = jnp.where(place == slots[n], wants[n] - holders[n] * TILES, named)
    wanted[...] = named.reshape(COLS, CAP, 128)

    pl.semaphore_wait(barrier, ROWS + COLS - 2)

    east = col_peer(1)
    north = row_peer(2)

    def to_col(a, b, sems, peer):
        return pltpu.make_async_remote_copy(
            a, b, sems[0], sems[1], device_id={"col": peer}, device_id_type=MESH
        )

    def to_row(a, b, sems, peer):
        return pltpu.make_async_remote_copy(
            a, b, sems[0], sems[1], device_id={"row": peer}, device_id_type=MESH
        )

    id_sems = (id_send.at[0], id_recv.at[0])

    def id_copy(peer):
        return to_col(wanted.at[peer], ids.at[col], id_sems, peer)

    def id_all_copies():
        rest = pl.ds(0, COLS - 1)
        return to_col(wanted.at[rest], ids.at[rest], id_sems, east)

    many = pl.ds(0, (COLS - 1) * 64)

    def f_copy(c, peer):
        sems = (f_send.at[c], f_recv.at[c])
        return to_col(fo.at[c, rows(peer, 64)], fr.at[c, rows(col, 64)], sems, peer)

    def f_all(c):
        return to_col(fo.at[c, many], fr.at[c, many], (f_send.at[c], f_recv.at[c]), east)

    def b_copy(c, peer):
        sems = (b_send.at[c], b_recv.at[c])
        return to_col(ro.at[c, rows(peer, 64)], ri.at[c, rows(col, 64)], sems, peer)

    def b_all(c):
        return to_col(ro.at[c, many], ri.at[c, many], (b_send.at[c], b_recv.at[c]), east)

    def r_rows(n, peer):
        return pl.ds(pl.multiple_of((peer * 4 + 2 * lax.rem(n, 2)) * 128, 256), 256)

    def r_copy(n, peer):
        sems = (r_send.at[n], r_recv.at[n])
        return to_row(v.at[n // 2, r_rows(n, peer)], g.at[n, rows(row, 256)], sems, peer)

    def r_all(n):
        most = pl.ds(0, (ROWS - 1) * 256)
        return to_row(v.at[n // 2, most], g.at[n, most], (r_send.at[n], r_recv.at[n]), north)

    def c_copy(n, peer):
        sems = (c_send.at[n], c_recv.at[n])
        return to_col(s.at[n, rows(peer, 128)], h.at[n, rows(col, 128)], sems, peer)

    def c_all(n):
        most = pl.ds(0, (COLS - 1) * 128)
        return to_col(s.at[n, most], h.at[n, most], (c_send.at[n], c_recv.at[n]), east)

    def each_col(do):
        def step(d, _):
            do(col_peer(d))
            return 0

        lax.fori_loop(1, COLS, step, 0)

    def each_row(do):
        def step(d, _):
            do(row_peer(d))
            return 0

        lax.fori_loop(1, ROWS, step, 0)

    each_col(lambda p: id_copy(p).start())
    ids[col] = wanted[col]

    for load in loads[1:4] + loads[8:10]:
        load.wait()
    def prepare(b, _):
        hi, lo = split(vert[b])
        vth[b] = hi
        vtl[b] = lo
        for k in range(K):
            weight[b, k * TY : (k + 1) * TY, :] = amp[b, k : k + 1, :] * lat[b]
        return 0

    lax.fori_loop(0, 8, prepare, 0)

    wide = lax.broadcasted_iota(jnp.int32, (2 * TY, SLOTS * TY), 1)
    deep = lax.broadcasted_iota(jnp.int32, (2 * TY, SLOTS * TY), 0)
    for n in range(0, REQ, 2):
        cell = jnp.where(deep < TY, slots[n] * TY + deep, slots[n + 1] * TY + deep - TY)
        take[n * TY : (n + 2) * TY, :] = jnp.where(wide == cell, 1.0, 0.0).astype(BF16)
    across = lax.broadcasted_iota(jnp.int32, (8, REQ * TY), 1)
    cell = jnp.zeros((8, REQ * TY), jnp.int32)
    for n in range(REQ):
        cell = jnp.where(lax.shift_right_logical(across, 3) == n, slots[n] * TY, cell)
    cell = jnp.broadcast_to((cell + (across & 7))[0:1], (128, REQ * TY))
    down = lax.broadcasted_iota(jnp.int32, (128, REQ * TY), 0)

    def build(i, _):
        give[rows(i, 128), :] = jnp.where(down + i * 128 == cell, 1.0, 0.0).astype(BF16)
        return 0

    lax.fori_loop(0, SLOTS * TY // 128, build, 0)

    hi, lo = split(table[...])
    tab_h[...] = hi
    tab_l[...] = lo
    for i in range(16):
        tw[i] = jnp.broadcast_to(tw_in[:, i : i + 1], (256, 128))

    loads[4].wait()
    id_all_copies().wait_recv()
    id_all = ids[...].reshape(SLOTS, 128)
    for j in range(4):
        hit = jnp.where(id_all == lane + 128 * j, 1.0, 0.0).astype(F32)
        at = slice(j * 128, (j + 1) * 128)
        pick[:, at] = hit.astype(BF16)

    def pair(ref, c, q, n):
        a = ref[c, pl.ds(2 * q, n, stride=TY), :]
        b = ref[c, pl.ds(2 * q + 1, n, stride=TY), :]
        return split(jnp.concatenate([a, b], axis=1))

    def gather(c):
        for q in range(4):
            hi, lo = pair(v, c, q, TILES)
            got = dot(pick[...], hi) + dot(pick[...], lo)
            for e in range(2):
                fo[c, pl.ds(2 * q + e, SLOTS, stride=TY), :] = got[:, e * 128 : (e + 1) * 128]
        each_col(lambda p: f_copy(c, p).start())
        fr[c, rows(col, 64), :] = fo[c, rows(col, 64), :]

    gather(0)
    gather(1)
    for j in range(4):
        hit = jnp.where(id_all == lane + 128 * j, 1.0, 0.0).astype(F32).T.astype(BF16)
        at = slice(j * 128, (j + 1) * 128)
        put[at, 0:128] = hit
        put[at, 128:256] = hit

    for load in loads[5:8] + loads[10:]:
        load.wait()

    def cut(i, _):
        at = rows(i, 128)
        for j in range(4):
            hi, lo = split(zf[at, j * 256 : (j + 1) * 256])
            zh[j, at, :] = hi
            zl[j, at, :] = lo
        return 0

    lax.fori_loop(0, 8, cut, 0)

    def markers(c):
        f_all(c).wait_recv()
        f_hi, f_lo = split(fr[c])
        mine = dot(take[...], f_hi) + dot(take[...], f_lo)
        for b in range(8):
            own = [slice((k * 8 + b) * TY, (k * 8 + b + 1) * TY) for k in range(K)]
            p_hi, p_lo = split(jnp.concatenate([mine[at, :] for at in own], axis=0))
            inner = dot(p_hi, vth[b]) + (dot(p_lo, vth[b]) + dot(p_hi, vtl[b]))
            w = weight[b]
            sampled = jnp.sum(w * inner, axis=0, keepdims=True)
            force = wall[c, b : b + 1, :] - sampled
            force_out[c, b : b + 1, :] = force
            s_hi, s_lo = split(w * (surf[b : b + 1, :] * force))
            last = ((1,), (1,))
            back = dot(s_hi, vth[b], last) + (dot(s_lo, vth[b], last) + dot(s_hi, vtl[b], last))
            for k in range(K):
                spread[own[k], :] = back[k * TY : (k + 1) * TY, :]
        b_hi, b_lo = split(spread[...])
        ro[c] = dot(give[...], b_hi) + dot(give[...], b_lo)
        each_col(lambda p: b_copy(c, p).start())
        ri[c, rows(col, 64), :] = ro[c, rows(col, 64), :]

    def row_sends(n):
        each_row(lambda p: r_copy(n, p).start())
        g[n, rows(row, 256), :] = v[n // 2, r_rows(n, row), :]

    def force_tiles(c):
        b_all(c).wait_recv()
        for q in range(4):
            hi, lo = pair(ri, c, q, SLOTS)
            delta = dot(put[...], jnp.concatenate([hi, lo], axis=0))
            for e in range(2):
                at = pl.ds(2 * q + e, TILES, stride=TY)
                v[c, at, :] = v[c, at, :] + delta[:, e * 128 : (e + 1) * 128]
        pl.when(c < 2)(lambda: row_sends(c))

    low = lane < 64

    def axial(n):
        r_all(n).wait_recv()

        @pl.when(n == 1)
        def _():
            row_sends(2)

        for r in range(ROWS):
            hi, lo = split(g[n, r * 256 : (r + 1) * 256, :])
            xh[0:256, r * 128 : (r + 1) * 128] = hi
            xh[256:512, r * 128 : (r + 1) * 128] = lo

        def tile(turn, _):
            j = lax.rem(z + turn, 4)
            acc = dot(xh[...], zh[j])
            acc = acc[0:256] + (acc[256:512] + dot(xh[0:256, :], zl[j]))
            for t in range(2):
                a0 = acc[0:128, t * 128 : (t + 1) * 128]
                a1 = acc[128:256, t * 128 : (t + 1) * 128]
                s[n, rows(4 * j + 2 * t, 128), :] = jnp.where(low, a0, pltpu.roll(a1, 64, 1))
                s[n, rows(4 * j + 2 * t + 1, 128), :] = jnp.where(low, pltpu.roll(a0, 64, 1), a1)

            def send(d, _):
                @pl.when(4 * turn + d > 0)
                def _():
                    c_copy(n, 4 * j + lax.rem(y + d, 4)).start()

                return 0

            lax.fori_loop(0, 4, send, 0)
            return 0

        lax.fori_loop(0, 4, tile, 0)
        h[n, rows(col, 128), :] = s[n, rows(col, 128), :]

        @pl.when((n > 0) & (n < 4))
        def _():
            row_sends(n + 2)

    half = np.float32(np.sqrt(0.5))

    def fourier(n):
        c_all(n).wait_recv()
        for q in range(4):
            a = h[n, pl.ds(2 * q, 256, stride=8), :]
            b = h[n, pl.ds(2 * q + 1, 256, stride=8), :]
            hi, lo = split(jnp.concatenate([a, b], axis=1))
            acc = dot(tab_h[...], hi) + (dot(tab_h[...], lo) + dot(tab_l[...], hi))
            u[2 * q] = acc[:, 0:128]
            u[2 * q + 1] = acc[:, 128:256]

        def combine(i, _):
            re = rows(i, 8)
            im = pl.ds(pl.multiple_of(256 + i * 8, 8), 8)
            a = []
            for m in range(8):
                ur, ui = u[m, re, :], u[m, im, :]
                if m > 0:
                    tc, ts = tw[m, re, :], tw[8 + m, re, :]
                    ur, ui = ur * tc + ui * ts, ui * tc - ur * ts
                a.append((ur, ui))

            def add(p, q):
                return (p[0] + q[0], p[1] + q[1])

            def sub(p, q):
                return (p[0] - q[0], p[1] - q[1])

            def turn(p):
                return (p[1], -p[0])

            def four(p, q, r, t):
                s0, d0, s1, d1 = add(p, r), sub(p, r), add(q, t), turn(sub(q, t))
                return add(s0, s1), add(d0, d1), sub(s0, s1), sub(d0, d1)

            e0, e1, e2, e3 = four(a[0], a[2], a[4], a[6])
            o0, o1, o2, o3 = four(a[1], a[3], a[5], a[7])
            o1 = ((o1[0] + o1[1]) * half, (o1[1] - o1[0]) * half)
            o3 = ((o3[1] - o3[0]) * half, (-o3[1] - o3[0]) * half)
            for k2, (e, o) in enumerate(((e0, o0), (e1, o1), (e2, turn(o2)), (e3, o3))):
                xr, xi = add(e, o)
                xk[0, k2, re, :] = xr
                xk[1, k2, re, :] = xi
            return 0

        lax.fori_loop(0, 32, combine, 0, unroll=2)
        for p in range(2):
            for k2 in range(4):
                at = slice(k2 * 256, (k2 + 1) * 256)
                out[p, n // 2, lax.rem(n, 2), :, at] = xk[p, k2].T * damp[:, at]

    def step(i, _):
        @pl.when(i < 3)
        def _():
            markers(i)

        @pl.when(i == 0)
        def _():
            gather(2)

        @pl.when((i > 2) & (i < 3 + CHUNKS))
        def _():
            axial(i - 3)

        @pl.when((i > 0) & (i < 4))
        def _():
            force_tiles(i - 1)

        @pl.when(i > 3)
        def _():
            fourier(i - 4)

        return 0

    lax.fori_loop(0, CHUNKS + 4, step, 0)

    id_all_copies().wait_send()
    for c in range(3):
        f_all(c).wait_send()
        b_all(c).wait_send()
    for n in range(CHUNKS):
        r_all(n).wait_send()
        c_all(n).wait_send()


def local(velocity, z_inverse, tiles, amplitude, lateral, vertical, wall_velocity, surface):
    table, twiddle, damping = tables()
    any_ = pl.BlockSpec(memory_space=pl.ANY)
    vmem = pl.BlockSpec(memory_space=pltpu.VMEM)
    dma = pltpu.SemaphoreType.DMA
    spectrum, force = pl.pallas_call(
        kernel,
        out_shape=(
            pltpu.VMEM((2, 3, 2, 128, 1024), F32),
            pltpu.VMEM((3, 8, 256), F32),
        ),
        in_specs=[any_] * 11,
        out_specs=(vmem, vmem),
        scratch_shapes=[
            pltpu.SMEM((4, 8), jnp.int32),
            pltpu.VMEM((8, 4, 256), F32),
            pltpu.VMEM((8, 8, 256), F32),
            pltpu.VMEM((8, 128, 256), F32),
            pltpu.VMEM((3, 8, 256), F32),
            pltpu.VMEM((8, 256), F32),
            pltpu.VMEM((512, 256), F32),
            pltpu.VMEM((256, 128), F32),
            pltpu.VMEM((1, 1024), F32),
            pltpu.VMEM((COLS, CAP, 128), jnp.int32),
            pltpu.VMEM((3, 4096, 128), F32),
            pltpu.VMEM((1024, 1024), F32),
            pltpu.VMEM((4, 1024, 256), BF16),
            pltpu.VMEM((4, 1024, 256), BF16),
            pltpu.VMEM((8, 128, 256), BF16),
            pltpu.VMEM((8, 128, 256), BF16),
            pltpu.VMEM((8, 32, 256), F32),
            pltpu.VMEM((512, 256), BF16),
            pltpu.VMEM((512, 256), BF16),
            pltpu.VMEM((16, 256, 128), F32),
            pltpu.VMEM((COLS, CAP, 128), jnp.int32),
            pltpu.VMEM((SLOTS, TILES), BF16),
            pltpu.VMEM((TILES, 2 * SLOTS), BF16),
            pltpu.VMEM((REQ * TY, SLOTS * TY), BF16),
            pltpu.VMEM((SLOTS * TY, REQ * TY), BF16),
            pltpu.VMEM((3, SLOTS * TY, 128), F32),
            pltpu.VMEM((3, SLOTS * TY, 128), F32),
            pltpu.VMEM((REQ * TY, 128), F32),
            pltpu.VMEM((3, SLOTS * TY, 128), F32),
            pltpu.VMEM((3, SLOTS * TY, 128), F32),
            pltpu.VMEM((CHUNKS, ROWS * 256, 128), F32),
            pltpu.VMEM((512, 1024), BF16),
            pltpu.VMEM((CHUNKS, NY, 128), F32),
            pltpu.VMEM((CHUNKS, NY, 128), F32),
            pltpu.VMEM((8, 512, 128), F32),
            pltpu.VMEM((2, 4, 256, 128), F32),
            dma((11,)), dma((1,)), dma((1,)),
            dma((3,)), dma((3,)), dma((3,)), dma((3,)),
            dma((CHUNKS,)), dma((CHUNKS,)), dma((CHUNKS,)), dma((CHUNKS,)),
        ],
        compiler_params=pltpu.CompilerParams(
            collective_id=0, has_side_effects=True, vmem_limit_bytes=53 * 1024 * 1024
        ),
        name="slab",
    )(
        velocity.reshape(3, 4096, 128), z_inverse, tiles.T, amplitude, lateral, vertical, wall_velocity.transpose(1, 0, 2), surface,
        jnp.asarray(table), jnp.asarray(twiddle), jnp.asarray(damping),
    )
    return (spectrum.reshape(2, 3, 4, 64, 1024), force.transpose(1, 0, 2))


def solution(mesh):
    in_specs = (
        P(None, None, "col", "row"),
        P(),
        P(("row", "col"), None),
        P(("row", "col"), None, None),
        P(("row", "col"), None, None),
        P(("row", "col"), None, None),
        P(("row", "col"), None, None),
        P(("row", "col"), None),
    )
    out_specs = (P(None, None, "row", "col", None), P(("row", "col"), None, None))
    return jax.shard_map(local, mesh=mesh, in_specs=in_specs, out_specs=out_specs, check_vma=False)
```
